32 devices in a mesh: ctx: 8 (over y, x, core), head: 4 (over z).
Axes of the slice: x: 2, y: 2, z: 4, core: 2. Of those that a mesh axis runs over, the one named last changes fastest.
Arguments:
- tokens: bfloat16 [2048, 3072], P('ctx', 'head'), may hold values from -6 to 6
- w_qkv: bfloat16 [3, 3072, 3072], P(None, None, 'head'), may hold values from -0.109375 to 0.109375
- w_out: bfloat16 [3072, 3072], P('head'), may hold values from -2 to 2
- block_perm: int32 [32], replicated, may hold values from 0 to 31, as said below
Outputs:
- mixed: bfloat16 [2048, 3072], P('ctx', 'head')
The draws below stay inside these ranges and needn't reach their ends.
Inputs may be any that keep to these rules, and one draw needn't show every extreme that they name: A permutation; slot s holds frame row block_perm[s], token rows s * 64 to (s + 1) * 64 - 1 of tokens. Cut the frame rows into 16 runs of 2 consecutive rows, numbered 0 up; each index of ctx holds, for one c of its own, run c in its first 2 slots and run 2 * 8 - 1 - c in its last 2 slots, in row order.
All inputs are finite; a program needn't handle non-finite values.
Results may differ from the reference program's by a relative error of at most 0.02.
Values may be sent and summed in bfloat16 or wider, within the bound.
No kernel may reach another device: no remote copies, remote signals or barrier semaphores. Data moves between devices by JAX's collectives and lax.ppermute only.
A program may use at most 192 MiB of HBM per device.

```python
import jax
import jax.numpy as jnp
from jax import lax

D = 3072
HEADS = 24
HD = 128
WW = 64
F = 8
BPD = 4
NB = 32
TOKENS = 2048


def draw_block_perm(key, part):
    holders = NB // BPD
    run_len = BPD // 2
    order = jax.random.permutation(key, holders).astype(jnp.int32)
    slot_ids = jnp.arange(NB, dtype=jnp.int32)
    holder = slot_ids // BPD
    inside = slot_ids % BPD
    run_id = order[holder]
    early = run_id * run_len + inside
    late = (2 * holders - 1 - run_id) * run_len + inside - run_len
    return jnp.where(inside < run_len, early, late).astype(jnp.int32)


def levels(rng, shape, shards, smallest, top_value):
    def one(axis_at, shards_of):
        draws = jax.random.uniform(jax.random.fold_in(jax.random.fold_in(rng, 6), axis_at), (shards_of,), jnp.float32, smallest / len(shards), top_value / len(shards))
        return jnp.repeat(jnp.exp(draws), shape[axis_at] // shards_of).reshape((-1,) + (1,) * (len(shape) - axis_at - 1))

    factor_of = one(*shards[0])
    for cut in shards[1:]:
        factor_of = factor_of * one(*cut)
    return factor_of


def bell_draw(stream_key, dims, scale, limit, cuts=(), held_as=jnp.bfloat16):
    values = jax.random.normal(stream_key, dims, jnp.float32) * scale
    if len(cuts) > 0:
        values = levels(stream_key, dims, cuts, -0.22, 0.18) * values
    return jnp.clip(values, min=-limit, max=limit).astype(held_as)


def setup_inputs(seed: int = 0) -> dict:
    keys = jax.random.split(jax.random.key(seed), 5)
    return {
        "tokens": bell_draw(keys[0], (TOKENS, D), 1.0, 6.0, ((0, 8), (1, 4))),
        "w_qkv": bell_draw(keys[1], (3, D, D), D ** -0.5, 0.109375, ((2, 4),)),
        "w_out": bell_draw(keys[2], (D, D), (HD // 16) ** -0.5, 2.0, ((0, 4),)),
        "block_perm": draw_block_perm(jax.random.fold_in(keys[4], 71), 0),
    }


ROPE_BASE = 10000.0
EPSILON = 1e-06

def frames_and_rows(block_perm, frame_total):
    frame_rows = block_perm.shape[0] // frame_total
    slot_frame = (block_perm // frame_rows).astype(jnp.int32)
    slot_row = (block_perm % frame_rows).astype(jnp.int32)
    return (slot_frame, slot_row)

def rope_angles(frame_of_block, row_of_block, block_width, head_size):
    grid_shape = (frame_of_block.shape[0], block_width)
    pos_frame = jnp.broadcast_to(frame_of_block[:, None], grid_shape).reshape(-1).astype(jnp.float32)
    pos_row = jnp.broadcast_to(row_of_block[:, None], grid_shape).reshape(-1).astype(jnp.float32)
    pos_column = jnp.broadcast_to(jnp.arange(block_width, dtype=jnp.int32)[None, :], grid_shape).reshape(-1).astype(jnp.float32)
    pair_counts = (head_size // 16, 7 * head_size // 32, 7 * head_size // 32)
    angle_parts = []
    for position, pair_count in zip((pos_frame, pos_row, pos_column), pair_counts):
        frequency = ROPE_BASE ** (-jnp.arange(pair_count, dtype=jnp.float32) / pair_count)
        angle_parts.append(position[:, None] * frequency[None, :])
    return angle_parts

def normalize(vector):
    return vector * lax.rsqrt(lax.optimization_barrier(jnp.mean(vector * vector, axis=-1, keepdims=True)) + EPSILON)

def rotate(vector, angle_parts):
    pieces = []
    offset = 0
    for angle_part in angle_parts:
        pair_count = angle_part.shape[1]
        lower_half = vector[..., offset:offset + pair_count]
        upper_half = vector[..., offset + pair_count:offset + 2 * pair_count]
        cosine = jnp.cos(angle_part)[:, None, :]
        sine_part = jnp.sin(angle_part)[:, None, :]
        pieces.append(lower_half * cosine - upper_half * sine_part)
        pieces.append(lower_half * sine_part + upper_half * cosine)
        offset = offset + 2 * pair_count
    return jnp.concatenate(pieces, axis=-1)

def reference(tokens, w_qkv, w_out, block_perm):
    tok_total = tokens.shape[0]
    slot_frame, slot_row = frames_and_rows(block_perm, F)
    angle_parts = rope_angles(slot_frame, slot_row, WW, HD)
    query_raw = jnp.dot(tokens, w_qkv[0], preferred_element_type=jnp.float32).reshape(tok_total, HEADS, HD)
    key_raw = jnp.dot(tokens, w_qkv[1], preferred_element_type=jnp.float32).reshape(tok_total, HEADS, HD)
    value_data = jnp.dot(tokens, w_qkv[2], preferred_element_type=jnp.float32).astype(jnp.bfloat16).reshape(tok_total, HEADS, HD)
    q_rot = rotate(normalize(query_raw), angle_parts).astype(jnp.bfloat16)
    k_rot = rotate(normalize(key_raw), angle_parts).astype(jnp.bfloat16)
    block_ok = (slot_frame[None, :] <= slot_frame[:, None]).astype(jnp.float32)
    slots = slot_frame.shape[0]
    token_ok = jnp.broadcast_to(block_ok[:, None, :, None], (slots, WW, slots, WW)).reshape(tok_total, tok_total)

    def one_head(head_id):
        query_head = lax.dynamic_index_in_dim(q_rot, head_id, 1, keepdims=False)
        key_head = lax.dynamic_index_in_dim(k_rot, head_id, 1, keepdims=False)
        value_head = lax.dynamic_index_in_dim(value_data, head_id, 1, keepdims=False)
        scores = jnp.dot(query_head, key_head.T, preferred_element_type=jnp.float32) * HD ** (-0.5)
        weights = jnp.exp(scores) * token_ok
        denominator = lax.optimization_barrier(jnp.sum(weights, axis=1))
        numerator = jnp.dot(weights.astype(jnp.bfloat16), value_head, preferred_element_type=jnp.float32)
        return (numerator / denominator[:, None]).astype(jnp.bfloat16)
    per_head = lax.map(one_head, jnp.arange(HEADS, dtype=jnp.int32))
    attention = jnp.transpose(per_head, (1, 0, 2)).reshape(tok_total, HEADS * HD)
    return jnp.dot(attention, w_out, preferred_element_type=jnp.float32).astype(jnp.bfloat16)
```

```python
import functools
import math

import jax
import jax.numpy as jnp
from jax import lax
from jax.experimental import pallas as pl
from jax.experimental.pallas import tpu as pltpu
from jax.sharding import PartitionSpec as P

HD = 128
WW = 64
F = 8
ROPE_BASE = 10000.0
EPSILON = 1e-06
CORES = 2
MASKED = -1e30


def part_sizes():
    return (HD // 16, 7 * HD // 32, 7 * HD // 32)


def rope_tables(slot_frame, slot_row):
    slots = slot_frame.shape[0]
    lane = lax.broadcasted_iota(jnp.int32, (slots, WW, HD), 2)
    column = lax.broadcasted_iota(jnp.int32, (slots, WW, HD), 1).astype(jnp.float32)
    frame = jnp.broadcast_to(slot_frame.astype(jnp.float32)[:, None, None], lane.shape)
    row = jnp.broadcast_to(slot_row.astype(jnp.float32)[:, None, None], lane.shape)
    p0, p1, p2 = part_sizes()
    first, second = 2 * p0, 2 * p0 + 2 * p1
    position = jnp.where(lane < first, frame, jnp.where(lane < second, row, column))
    freq, sign = [], []
    for pairs in (p0, p1, p2):
        steps = ROPE_BASE ** (-jnp.arange(pairs, dtype=jnp.float32) / pairs)
        freq += [steps, steps]
        sign += [-jnp.ones((pairs,), jnp.float32), jnp.ones((pairs,), jnp.float32)]
    angle = position * jnp.concatenate(freq)
    cosine = jnp.cos(angle).reshape(slots * WW, HD)
    sine = (jnp.sin(angle) * jnp.concatenate(sign)).reshape(slots * WW, HD)
    return cosine, sine


def norm_rotate(v, cosine, sine, scale):
    p0, p1, _ = part_sizes()
    mean = jnp.mean(v * v, axis=-1, keepdims=True)
    v = v * (lax.rsqrt(mean + EPSILON) * scale)
    lane = lax.broadcasted_iota(jnp.int32, v.shape, 1)
    low = (
        (lane < p0)
        | ((lane >= 2 * p0) & (lane < 2 * p0 + p1))
        | ((lane >= 2 * p0 + 2 * p1) & (lane < 2 * p0 + 3 * p1))
    )
    near = jnp.where(low, pltpu.roll(v, HD - p0, 1), pltpu.roll(v, p0, 1))
    far = jnp.where(low, pltpu.roll(v, HD - p1, 1), pltpu.roll(v, p1, 1))
    other = jnp.where(lane < 2 * p0, near, far)
    return v * cosine + other * sine


def project_kernel(pieces, heads, order_ref, *refs):
    mine = refs[:pieces]
    theirs = refs[pieces : 2 * pieces]
    w_ref, cos_ref, sin_ref, q_ref, kv_ref, acc = refs[2 * pieces :]
    step = pl.program_id(0)
    rows = mine[0].shape[0]
    for i in range(pieces):

        @pl.when(step == i)
        def _(i=i):
            for j in range(3):
                for r, part in enumerate((mine[i], theirs[i])):
                    dot = jnp.dot(part[...], w_ref[j], preferred_element_type=jnp.float32)
                    window = (j, pl.ds(r * rows, rows))
                    if i == 0:
                        acc[window] = dot
                    else:
                        acc[window] += dot

    @pl.when(step == pieces - 1)
    def _():
        width = heads * HD
        for r in range(2):
            window = pl.ds(r * rows, rows)
            cosine, sine = cos_ref[window], sin_ref[window]
            for h in range(heads):
                cols = pl.ds(h * HD, HD)
                scale = HD ** (-0.5) * math.log2(math.e)
                q = norm_rotate(acc[0, window, cols], cosine, sine, scale)
                k = norm_rotate(acc[1, window, cols], cosine, sine, 1.0)
                q_ref[window, cols] = q.astype(jnp.bfloat16)
                kv_ref[window, cols] = k.astype(jnp.bfloat16)
            kv_ref[window, pl.ds(width, width)] = acc[2, window].astype(jnp.bfloat16)


def project(order, mine, theirs, w_qkv, cosine, sine):
    pieces = len(mine)
    rows, feats = mine[0].shape
    width = w_qkv.shape[2] // CORES
    heads = width // HD
    whole = lambda shape: pl.BlockSpec(shape, lambda i, o: (0,) * len(shape))
    grid_spec = pltpu.PrefetchScalarGridSpec(
        num_scalar_prefetch=1,
        grid=(pieces,),
        in_specs=[whole((rows, feats))] * (2 * pieces)
        + [
            pl.BlockSpec((3, feats, width), lambda i, o: (0, o[i], o[pieces])),
            whole(cosine.shape),
            whole(sine.shape),
        ],
        out_specs=[whole((2 * rows, width)), whole((2 * rows, 2 * width))],
        scratch_shapes=[pltpu.VMEM((3, 2 * rows, width), jnp.float32)],
    )
    return pl.pallas_call(
        functools.partial(project_kernel, pieces, heads),
        grid_spec=grid_spec,
        out_shape=[
            jax.ShapeDtypeStruct((2 * rows, width), jnp.bfloat16),
            jax.ShapeDtypeStruct((2 * rows, 2 * width), jnp.bfloat16),
        ],
        cost_estimate=pl.CostEstimate(
            flops=2 * 2 * rows * feats * pieces * 3 * width,
            bytes_accessed=3 * feats * pieces * width * 2,
            transcendentals=0,
        ),
        name="project",
    )(order, *mine, *theirs, w_qkv, cosine, sine)


def attend_kernel(free, masked, heads, bias_ref, q_ref, *refs):
    total = free + masked
    kv = refs[:total]
    out_ref = refs[total]
    rows = q_ref.shape[0] // 2
    width = heads * HD
    for h in range(heads):
        cols = pl.ds(h * HD, HD)
        for r in range(2):
            window = pl.ds(r * rows, rows)
            q = q_ref[window, cols]
            acc = jnp.zeros((rows, 2 * HD), jnp.float32)
            for i in range(total):
                keys = kv[i][:, cols]
                values = kv[i][:, pl.ds(width + h * HD, HD)]
                scores = lax.dot_general(
                    q, keys, (((1,), (1,)), ((), ())), preferred_element_type=jnp.float32
                )
                if i >= free:
                    half = scores.shape[1] // 2
                    at = 2 * (i - free)
                    scores = jnp.concatenate(
                        [
                            scores[:, :half] + bias_ref[r, at],
                            scores[:, half:] + bias_ref[r, at + 1],
                        ],
                        axis=1,
                    )
                weights = jnp.exp2(scores).astype(jnp.bfloat16)
                wide = jnp.concatenate([values, jnp.ones_like(values)], axis=1)
                acc += jnp.dot(weights, wide, preferred_element_type=jnp.float32)
            out_ref[window, cols] = (acc[:, :HD] / acc[:, HD:]).astype(jnp.bfloat16)


def attend(bias, q, free, masked):
    rows2, width = q.shape
    heads = width // HD
    keys = sum(p.shape[0] for p in free + masked)
    vmem = pl.BlockSpec(memory_space=pltpu.VMEM)
    return pl.pallas_call(
        functools.partial(attend_kernel, len(free), len(masked), heads),
        in_specs=[pl.BlockSpec(memory_space=pltpu.SMEM)]
        + [vmem] * (1 + len(free) + len(masked)),
        out_specs=vmem,
        out_shape=jax.ShapeDtypeStruct((rows2, width), jnp.bfloat16),
        cost_estimate=pl.CostEstimate(
            flops=8 * rows2 * keys * width, bytes_accessed=4 * keys * width, transcendentals=0
        ),
        name="attend",
    )(bias, q, *free, *masked)


def output_kernel(blocks, order_ref, mine_ref, theirs_ref, w_ref, *outs):
    step = pl.program_id(0)
    width = mine_ref.shape[1]
    mine_at = pl.multiple_of(order_ref[blocks] * width, width)
    theirs_at = pl.multiple_of(order_ref[blocks + 1] * width, width)
    part = jnp.dot(
        mine_ref[...], w_ref[pl.ds(mine_at, width)], preferred_element_type=jnp.float32
    ) + jnp.dot(
        theirs_ref[...], w_ref[pl.ds(theirs_at, width)], preferred_element_type=jnp.float32
    )
    for i in range(blocks):

        @pl.when(step == i)
        def _(i=i):
            outs[i][...] = part.astype(outs[i].dtype)


def output_parts(order, mine, theirs, w_out, blocks):
    rows, width = mine.shape
    cols = w_out.shape[1] // blocks
    whole = lambda shape: pl.BlockSpec(shape, lambda i, o: (0,) * len(shape))
    grid_spec = pltpu.PrefetchScalarGridSpec(
        num_scalar_prefetch=1,
        grid=(blocks,),
        in_specs=[
            whole((rows, width)),
            whole((rows, width)),
            pl.BlockSpec((w_out.shape[0], cols), lambda i, o: (0, o[i])),
        ],
        out_specs=[whole((rows, cols))] * blocks,
    )
    return pl.pallas_call(
        functools.partial(output_kernel, blocks),
        grid_spec=grid_spec,
        out_shape=[
            jax.ShapeDtypeStruct((rows, cols), jnp.bfloat16 if i < blocks - 1 else jnp.float32)
            for i in range(blocks)
        ],
        cost_estimate=pl.CostEstimate(
            flops=2 * rows * w_out.shape[0] * w_out.shape[1],
            bytes_accessed=w_out.shape[0] * w_out.shape[1] * 2,
            transcendentals=0,
        ),
        name="output_parts",
    )(order, mine, theirs, w_out)


def per_device(ctx, levels, tokens, w_qkv, w_out, block_perm):
    rows = tokens.shape[0]
    half = rows // 2
    local_slots = rows // WW
    run_slots = local_slots // 2
    me = lax.axis_index("ctx")
    level = lax.axis_index("head")
    core = me % CORES
    chips = ctx // CORES
    frame_rows = block_perm.shape[0] // F
    slot_frame = block_perm // frame_rows
    slot_row = block_perm % frame_rows

    shifts = list(range(1, levels))
    shifts.sort(key=lambda k: (-min(k, levels - k), k))

    def over_levels(x, k):
        return lax.ppermute(x, "head", [(i, (i + k) % levels) for i in range(levels)])

    def over_ctx(x, mask):
        return lax.ppermute(x, "ctx", [(i, i ^ mask) for i in range(ctx)])

    def slots_of(values, device, part):
        first = device * local_slots + part * run_slots
        return lax.dynamic_slice_in_dim(values, first, run_slots)

    def tables(part):
        frame = jnp.concatenate([slots_of(slot_frame, me, part), slots_of(slot_frame, me ^ 1, part)])
        row = jnp.concatenate([slots_of(slot_row, me, part), slots_of(slot_row, me ^ 1, part)])
        return rope_tables(frame, row)

    def run_frames(part):
        devices = jnp.stack([me ^ (2 * m + k) for m in range(chips) for k in range(2)])
        return slot_frame[devices * local_slots + part * run_slots]

    blocks = jnp.stack([level] + [(level - k) % levels for k in shifts] + [core]).astype(jnp.int32)

    projected = []
    for part in range(2):
        own = tokens[part * half : (part + 1) * half]
        mine = [own] + [over_levels(own, k) for k in shifts]
        theirs = [over_ctx(piece, 1) for piece in mine]
        cosine, sine = tables(part)
        projected.append(project(blocks, mine, theirs, w_qkv, cosine, sine))

    targets = jnp.stack(
        [(level + k) % levels for k in shifts] + [level, core, 1 - core]
    ).astype(jnp.int32)
    results = []
    free = []
    for part in range(2):
        q, kv = projected[part]
        pieces = [kv] + [over_ctx(kv, 2 * m) for m in range(1, chips)]
        frames = run_frames(part)
        bias = jnp.where(frames[None, :] <= frames[:2, None], 0.0, MASKED).astype(jnp.float32)
        mixed_heads = attend(bias, q, free, pieces)
        free = free + pieces
        mine = mixed_heads[:half]
        theirs = over_ctx(mixed_heads[half:], 1)
        parts = output_parts(targets, mine, theirs, w_out, levels)
        total = parts[-1]
        for k, partial in zip(shifts, parts):
            total = total + over_levels(partial, k).astype(jnp.float32)
        results.append(total.astype(jnp.bfloat16))
    return jnp.concatenate(results, axis=0)


def solution(mesh):
    in_specs = (P("ctx", "head"), P(None, None, "head"), P("head", None), P())
    out_specs = P("ctx", "head")
    body = functools.partial(per_device, mesh.shape["ctx"], mesh.shape["head"])
    return jax.shard_map(
        body, mesh=mesh, in_specs=in_specs, out_specs=out_specs, check_vma=False
    )
```

```python
import functools
import math

import jax
import jax.numpy as jnp
from jax import lax
from jax.experimental import pallas as pl
from jax.experimental.pallas import tpu as pltpu
from jax.sharding import PartitionSpec as P


HD = 128
WW = 64
F = 8
ROPE_BASE = 10000.0
EPSILON = 1e-06
CORES = 2
MASKED = -1e30
GRANT = 12 << 20


def part_sizes():
    return (HD // 16, 7 * HD // 32, 7 * HD // 32)


def rope_tables(slot_frame, slot_row):
    slots = slot_frame.shape[0]
    lane = lax.broadcasted_iota(jnp.int32, (slots, WW, HD), 2)
    column = lax.broadcasted_iota(jnp.int32, (slots, WW, HD), 1).astype(jnp.float32)
    frame = jnp.broadcast_to(slot_frame.astype(jnp.float32)[:, None, None], lane.shape)
    row = jnp.broadcast_to(slot_row.astype(jnp.float32)[:, None, None], lane.shape)
    p0, p1, p2 = part_sizes()
    first, second = 2 * p0, 2 * p0 + 2 * p1
    position = jnp.where(lane < first, frame, jnp.where(lane < second, row, column))
    freq, sign = [], []
    for pairs in (p0, p1, p2):
        steps = ROPE_BASE ** (-jnp.arange(pairs, dtype=jnp.float32) / pairs)
        freq += [steps, steps]
        sign += [-jnp.ones((pairs,), jnp.float32), jnp.ones((pairs,), jnp.float32)]
    angle = position * jnp.concatenate(freq)
    cosine = jnp.cos(angle).reshape(slots * WW, HD)
    sine = (jnp.sin(angle) * jnp.concatenate(sign)).reshape(slots * WW, HD)
    return cosine, sine


def norm_rotate(v, cosine, sine, scale):
    p0, p1, _ = part_sizes()
    mean = jnp.mean(v * v, axis=-1, keepdims=True)
    v = v * (lax.rsqrt(mean + EPSILON) * scale)
    lane = lax.broadcasted_iota(jnp.int32, v.shape, 1)
    low = (
        (lane < p0)
        | ((lane >= 2 * p0) & (lane < 2 * p0 + p1))
        | ((lane >= 2 * p0 + 2 * p1) & (lane < 2 * p0 + 3 * p1))
    )
    near = jnp.where(low, pltpu.roll(v, HD - p0, 1), pltpu.roll(v, p0, 1))
    far = jnp.where(low, pltpu.roll(v, HD - p1, 1), pltpu.roll(v, p1, 1))
    other = jnp.where(lane < 2 * p0, near, far)
    return v * cosine + other * sine


def vmem_call(body, inputs, outputs, smem=(), after=(), scratch=(), flops=0, grant=GRANT):
    vmem = pl.BlockSpec(memory_space=pltpu.VMEM)
    n_smem, n_after = len(smem), len(after)

    def kernel(*refs):
        body(*refs[:n_smem], *refs[n_smem + n_after :])

    single = len(outputs) == 1
    return pl.pallas_call(
        kernel,
        in_specs=[pl.BlockSpec(memory_space=pltpu.SMEM)] * n_smem
        + [pl.BlockSpec(memory_space=pl.ANY)] * n_after
        + [vmem] * len(inputs),
        out_specs=vmem if single else [vmem] * len(outputs),
        out_shape=outputs[0] if single else list(outputs),
        scratch_shapes=list(scratch),
        compiler_params=pltpu.CompilerParams(vmem_limit_bytes=grant),
        cost_estimate=pl.CostEstimate(flops=flops, bytes_accessed=0, transcendentals=0),
    )(*smem, *after, *inputs)


def fetch_kernel(cuts, *refs):
    count = len(cuts)
    sources, targets, sems = refs[:count], refs[count : 2 * count], refs[2 * count]
    core = lax.axis_index("ctx") % CORES
    copies = []
    for source, target, cut in zip(sources, targets, cuts):
        for at in range(target.shape[0]):
            view = source.at[at]
            if cut:
                width = target.shape[-1]
                cols = pl.ds(pl.multiple_of(core * width, width), width)
                view = source.at[at, :, cols]
            copies.append(pltpu.make_async_copy(view, target.at[at], sems.at[len(copies)]))
    for copy in copies:
        copy.start()
    for copy in copies:
        copy.wait()


def fetch(w_qkv, w_out, pieces):
    three, feats, cols = w_qkv.shape
    shapes = [(three, feats, cols // CORES), (pieces, w_out.shape[0] // pieces, w_out.shape[1])]
    any_space = pl.BlockSpec(memory_space=pltpu.MemorySpace.HBM)
    return pl.pallas_call(
        functools.partial(fetch_kernel, (True, False)),
        in_specs=[any_space] * 2,
        out_specs=[pl.BlockSpec(memory_space=pltpu.VMEM)] * 2,
        out_shape=[jax.ShapeDtypeStruct(shape, jnp.bfloat16) for shape in shapes],
        scratch_shapes=[pltpu.SemaphoreType.DMA((three + pieces,))],
        compiler_params=pltpu.CompilerParams(vmem_limit_bytes=46 << 20),
        name="fetch",
    )(w_qkv, w_out.reshape(shapes[1]))


def project_kernel(pieces, heads, shifts, kind, cos_ref, sin_ref, *refs):
    mine = refs[:pieces]
    theirs = refs[pieces : 2 * pieces]
    w_ref, out_ref = refs[2 * pieces :]
    _, feats = mine[0].shape
    width = heads * HD
    level = lax.axis_index("head")

    def product(j):
        total = None
        for i, k in enumerate(shifts):
            block = lax.rem(level - k + pieces, pieces)
            at = pl.ds(pl.multiple_of(block * feats, feats), feats)
            x = jnp.concatenate([mine[i][...], theirs[i][...]], axis=0)
            dot = jnp.dot(x, w_ref[j, at, :], preferred_element_type=jnp.float32)
            total = dot if total is None else total + dot
        return total

    scale = HD ** (-0.5) * math.log2(math.e) if kind == "q" else 1.0
    raw = product(0 if kind == "q" else 1)
    if kind == "kv":
        out_ref[:, pl.ds(width, width)] = product(2).astype(jnp.bfloat16)
    cosine, sine = cos_ref[...], sin_ref[...]
    for h in range(heads):
        v = norm_rotate(raw[:, h * HD : (h + 1) * HD], cosine, sine, scale)
        out_ref[:, pl.ds(h * HD, HD)] = v.astype(jnp.bfloat16)


def project(kind, shifts, mine, theirs, w_qkv, cosine, sine):
    pieces = len(mine)
    rows, feats = mine[0].shape
    width = w_qkv.shape[2]
    count = 1 if kind == "q" else 2
    return vmem_call(
        functools.partial(project_kernel, pieces, width // HD, shifts, kind),
        [cosine, sine, *mine, *theirs, w_qkv],
        [jax.ShapeDtypeStruct((2 * rows, count * width), jnp.bfloat16)],
        flops=2 * 2 * rows * feats * pieces * count * width,
    )


def attend_kernel(carried, final, free, masked, heads, part, local_slots, perm_ref, q_ref, *refs):
    state_ref = refs[0] if carried else None
    kv = refs[carried : carried + free + masked]
    out_ref = refs[-1]
    rows = q_ref.shape[0] // 2
    width = heads * HD
    frame_rows = perm_ref.shape[0] // F
    me = lax.axis_index("ctx")

    def frame(device):
        return perm_ref[device * local_slots + part * (local_slots // 2)] // frame_rows

    frames = [frame(me ^ m) for m in range(2 * masked)]
    for h in range(heads):
        cols = pl.ds(h * HD, HD)
        wide_cols = pl.ds(2 * h * HD, 2 * HD)
        for r in range(2):
            window = pl.ds(r * rows, rows)
            q = q_ref[window, cols]
            if carried:
                acc = state_ref[window, wide_cols]
            else:
                acc = jnp.zeros((rows, 2 * HD), jnp.float32)
            for i in range(free + masked):
                keys = kv[i][:, cols]
                values = kv[i][:, pl.ds(width + h * HD, HD)]
                scores = lax.dot_general(
                    q, keys, (((1,), (1,)), ((), ())), preferred_element_type=jnp.float32
                )
                if i >= free:
                    half = scores.shape[1] // 2
                    at = 2 * (i - free)
                    bias = [
                        jnp.where(frames[at + s] <= frames[r], jnp.float32(0), jnp.float32(MASKED))
                        for s in range(2)
                    ]
                    scores = jnp.concatenate(
                        [scores[:, :half] + bias[0], scores[:, half:] + bias[1]], axis=1
                    )
                weights = jnp.exp2(scores).astype(jnp.bfloat16)
                wide = jnp.concatenate([values, jnp.ones_like(values)], axis=1)
                acc += jnp.dot(weights, wide, preferred_element_type=jnp.float32)
            if final:
                out_ref[window, cols] = (acc[:, :HD] / acc[:, HD:]).astype(jnp.bfloat16)
            else:
                out_ref[window, wide_cols] = acc


def attend(block_perm, q, state, free, masked, part, local_slots, final):
    rows2, width = q.shape
    heads = width // HD
    keys = sum(p.shape[0] for p in free + masked)
    carried = 0 if state is None else 1
    if final:
        out = jax.ShapeDtypeStruct((rows2, width), jnp.bfloat16)
    else:
        out = jax.ShapeDtypeStruct((rows2, 2 * width), jnp.float32)
    return vmem_call(
        functools.partial(
            attend_kernel, carried, final, len(free), len(masked), heads, part, local_slots
        ),
        [q] + ([state] if carried else []) + free + masked,
        [out],
        smem=[block_perm],
        flops=8 * rows2 * keys * width,
    )


def output_kernel(shifts, mine_ref, theirs_ref, w_ref, *outs):
    levels = len(shifts)
    rows = theirs_ref.shape[0]
    width = mine_ref.shape[1]
    level = lax.axis_index("head")
    core = lax.axis_index("ctx") % CORES
    mine_at = pl.ds(pl.multiple_of(core * width, width), width)
    theirs_at = pl.ds(pl.multiple_of((1 - core) * width, width), width)
    mine = mine_ref[pl.ds(0, rows), :]
    theirs = theirs_ref[...]
    span = w_ref.shape[1] // levels
    for i, k in enumerate(shifts):
        block = lax.rem(level + k, levels)
        cols = pl.ds(pl.multiple_of(block * span, span), span)
        part = jnp.dot(mine, w_ref[mine_at, cols], preferred_element_type=jnp.float32)
        part += jnp.dot(theirs, w_ref[theirs_at, cols], preferred_element_type=jnp.float32)
        outs[i][...] = part.astype(outs[i].dtype)


def output_parts(shifts, mine, theirs, w_out):
    rows = theirs.shape[0]
    cols = w_out.shape[1] // len(shifts)
    return vmem_call(
        functools.partial(output_kernel, shifts),
        [mine, theirs, w_out],
        [
            jax.ShapeDtypeStruct((rows, cols), jnp.float32 if k == 0 else jnp.bfloat16)
            for k in shifts
        ],
        flops=2 * rows * w_out.shape[0] * w_out.shape[1],
    )


def finish_kernel(count, *refs):
    out_ref = refs[-1]
    rows = refs[0].shape[0]
    for part in range(2):
        group = refs[part * count : (part + 1) * count]
        total = group[0][...]
        for ref in group[1:]:
            total += ref[...].astype(jnp.float32)
        out_ref[pl.ds(part * rows, rows), :] = total.astype(out_ref.dtype)


def finish(first, second):
    rows, cols = first[0].shape
    return vmem_call(
        functools.partial(finish_kernel, len(first)),
        [*first, *second],
        [jax.ShapeDtypeStruct((2 * rows, cols), jnp.bfloat16)],
        flops=rows * cols,
    )


def per_device(ctx, levels, tokens, w_qkv, w_out, block_perm):
    rows = tokens.shape[0]
    half = rows // 2
    local_slots = rows // WW
    run_slots = local_slots // 2
    me = lax.axis_index("ctx")
    chips = ctx // CORES
    frame_rows = block_perm.shape[0] // F
    slot_frame = block_perm // frame_rows
    slot_row = block_perm % frame_rows

    shifts = sorted(range(1, levels), key=lambda k: (-min(k, levels - k), k))

    def over_levels(x, k):
        return lax.ppermute(x, "head", [(i, (i + k) % levels) for i in range(levels)])

    def over_ctx(x, mask):
        return lax.ppermute(x, "ctx", [(i, i ^ mask) for i in range(ctx)])

    def slots_of(values, device, part):
        first = device * local_slots + part * run_slots
        return lax.dynamic_slice_in_dim(values, first, run_slots)

    def tables(part):
        frame = jnp.concatenate([slots_of(slot_frame, me, part), slots_of(slot_frame, me ^ 1, part)])
        row = jnp.concatenate([slots_of(slot_row, me, part), slots_of(slot_row, me ^ 1, part)])
        return rope_tables(frame, row)

    turns = [tables(part) for part in range(2)]
    gathered = []
    for part in range(2):
        own = tokens[part * half : (part + 1) * half]
        pieces = [own]
        for k in shifts:
            pieces.append(over_levels(own, k))
        gathered.append(pieces)
    weights = fetch(w_qkv, w_out, levels)
    last, turns, weights = lax.optimization_barrier((gathered[0][-1], turns, weights))
    w_mine, w_rows = weights[0], weights[1].reshape(w_out.shape)
    gathered[0][-1] = last

    projected = []
    for part in range(2):
        mine = gathered[part]
        if part == 1:
            mine[1:], q = lax.optimization_barrier((mine[1:], q))
            projected[0] = (q, pieces)
        theirs = [over_ctx(piece, 1) for piece in mine]
        inputs = ([0] + shifts, mine, theirs, w_mine, *turns[part])
        kv = project("kv", *inputs)
        pieces = [kv]
        for m in range(1, chips):
            pieces.append(over_ctx(kv, 2 * m))
        q = project("q", *inputs)
        projected.append((q, pieces))

    sums = []
    for part in range(2):
        q, pieces = projected[part]
        state = None
        if part == 1:
            state = attend(block_perm, q, None, projected[0][1], [], part, local_slots, False)
            pieces[1:], state = lax.optimization_barrier((pieces[1:], state))
        heads_out = attend(block_perm, q, state, [], pieces, part, local_slots, True)
        theirs = over_ctx(heads_out[half:], 1)
        parts = output_parts(shifts + [0], heads_out, theirs, w_rows)
        arrived = []
        for k, p in zip(shifts, parts):
            arrived.append(over_levels(p, k))
        sums.append([parts[-1]] + arrived)
    return finish(*sums)


def solution(mesh):
    in_specs = (P("ctx", "head"), P(None, None, "head"), P("head", None), P())
    out_specs = P("ctx", "head")

    def body(*args):
        return per_device(mesh.shape["ctx"], mesh.shape["head"], *args)

    return jax.shard_map(
        body, mesh=mesh, in_specs=in_specs, out_specs=out_specs, check_vma=False
    )
```

```python
import functools
import math

import jax
import jax.numpy as jnp
from jax import lax
from jax.experimental import pallas as pl
from jax.experimental.pallas import tpu as pltpu
from jax.sharding import PartitionSpec as P


HD = 128
WW = 64
F = 8
ROPE_BASE = 10000.0
EPSILON = 1e-06
CORES = 2
MASKED = -1e30
GRANT = 12 << 20


def part_sizes():
    return (HD // 16, 7 * HD // 32, 7 * HD // 32)


def rope_tables(slot_frame, slot_row):
    slots = slot_frame.shape[0]
    lane = lax.broadcasted_iota(jnp.int32, (slots, WW, HD), 2)
    column = lax.broadcasted_iota(jnp.int32, (slots, WW, HD), 1).astype(jnp.float32)
    frame = jnp.broadcast_to(slot_frame.astype(jnp.float32)[:, None, None], lane.shape)
    row = jnp.broadcast_to(slot_row.astype(jnp.float32)[:, None, None], lane.shape)
    p0, p1, p2 = part_sizes()
    first, second = 2 * p0, 2 * p0 + 2 * p1
    position = jnp.where(lane < first, frame, jnp.where(lane < second, row, column))
    freq, sign = [], []
    for pairs in (p0, p1, p2):
        steps = ROPE_BASE ** (-jnp.arange(pairs, dtype=jnp.float32) / pairs)
        freq += [steps, steps]
        sign += [-jnp.ones((pairs,), jnp.float32), jnp.ones((pairs,), jnp.float32)]
    angle = position * jnp.concatenate(freq)
    cosine = jnp.cos(angle).reshape(slots * WW, HD)
    sine = (jnp.sin(angle) * jnp.concatenate(sign)).reshape(slots * WW, HD)
    return cosine, sine


def norm_rotate(v, cosine, sine, scale):
    p0, p1, _ = part_sizes()
    mean = jnp.mean(v * v, axis=-1, keepdims=True)
    v = v * (lax.rsqrt(mean + EPSILON) * scale)
    lane = lax.broadcasted_iota(jnp.int32, v.shape, 1)
    low = (
        (lane < p0)
        | ((lane >= 2 * p0) & (lane < 2 * p0 + p1))
        | ((lane >= 2 * p0 + 2 * p1) & (lane < 2 * p0 + 3 * p1))
    )
    near = jnp.where(low, pltpu.roll(v, HD - p0, 1), pltpu.roll(v, p0, 1))
    far = jnp.where(low, pltpu.roll(v, HD - p1, 1), pltpu.roll(v, p1, 1))
    other = jnp.where(lane < 2 * p0, near, far)
    return v * cosine + other * sine


def vmem_call(body, inputs, outputs, smem=(), after=(), scratch=(), flops=0, grant=GRANT):
    vmem = pl.BlockSpec(memory_space=pltpu.VMEM)
    n_smem, n_after = len(smem), len(after)

    def kernel(*refs):
        body(*refs[:n_smem], *refs[n_smem + n_after :])

    single = len(outputs) == 1
    return pl.pallas_call(
        kernel,
        in_specs=[pl.BlockSpec(memory_space=pltpu.SMEM)] * n_smem
        + [pl.BlockSpec(memory_space=pl.ANY)] * n_after
        + [vmem] * len(inputs),
        out_specs=vmem if single else [vmem] * len(outputs),
        out_shape=outputs[0] if single else list(outputs),
        scratch_shapes=list(scratch),
        compiler_params=pltpu.CompilerParams(vmem_limit_bytes=grant),
        cost_estimate=pl.CostEstimate(flops=flops, bytes_accessed=0, transcendentals=0),
    )(*smem, *after, *inputs)


def fetch_kernel(w_ref, out_ref, sems):
    width = out_ref.shape[2]
    core = lax.axis_index("ctx") % CORES
    cols = pl.ds(pl.multiple_of(core * width, width), width)
    copies = [
        pltpu.make_async_copy(w_ref.at[at, :, cols], out_ref.at[at], sems.at[at])
        for at in range(out_ref.shape[0])
    ]
    for copy in copies:
        copy.start()
    for copy in copies:
        copy.wait()


def fetch(w_qkv):
    three, feats, cols = w_qkv.shape
    return pl.pallas_call(
        fetch_kernel,
        in_specs=[pl.BlockSpec(memory_space=pltpu.MemorySpace.HBM)],
        out_specs=pl.BlockSpec(memory_space=pltpu.VMEM),
        out_shape=jax.ShapeDtypeStruct((three, feats, cols // CORES), jnp.bfloat16),
        scratch_shapes=[pltpu.SemaphoreType.DMA((three,))],
        compiler_params=pltpu.CompilerParams(vmem_limit_bytes=46 << 20),
        name="fetch",
    )(w_qkv)


def project_kernel(pieces, heads, shifts, kind, cos_ref, sin_ref, *refs):
    mine = refs[:pieces]
    theirs = refs[pieces : 2 * pieces]
    w_ref, out_ref = refs[2 * pieces :]
    _, feats = mine[0].shape
    width = heads * HD
    level = lax.axis_index("head")

    def product(j):
        total = None
        for i, k in enumerate(shifts):
            block = level ^ k
            at = pl.ds(pl.multiple_of(block * feats, feats), feats)
            x = jnp.concatenate([mine[i][...], theirs[i][...]], axis=0)
            dot = jnp.dot(x, w_ref[j, at, :], preferred_element_type=jnp.float32)
            total = dot if total is None else total + dot
        return total

    scale = HD ** (-0.5) * math.log2(math.e) if kind == "q" else 1.0
    raw = product(0 if kind == "q" else 1)
    if kind == "kv":
        out_ref[:, pl.ds(width, width)] = product(2).astype(jnp.bfloat16)
    cosine, sine = cos_ref[...], sin_ref[...]
    for h in range(heads):
        v = norm_rotate(raw[:, h * HD : (h + 1) * HD], cosine, sine, scale)
        out_ref[:, pl.ds(h * HD, HD)] = v.astype(jnp.bfloat16)


def project(kind, shifts, mine, theirs, w_qkv, cosine, sine):
    pieces = len(mine)
    rows, feats = mine[0].shape
    width = w_qkv.shape[2]
    count = 1 if kind == "q" else 2
    return vmem_call(
        functools.partial(project_kernel, pieces, width // HD, shifts, kind),
        [cosine, sine, *mine, *theirs, w_qkv],
        [jax.ShapeDtypeStruct((2 * rows, count * width), jnp.bfloat16)],
        flops=2 * 2 * rows * feats * pieces * count * width,
    )


def attend_kernel(
    carried, sides, final, free, masked, heads, part, local_slots, perm_ref, q_ref, *refs
):
    state_ref = refs[0] if carried else None
    kv = refs[carried : carried + free + masked]
    out_ref = refs[-1]
    rows = q_ref.shape[0] // 2
    width = heads * HD
    frame_rows = perm_ref.shape[0] // F
    me = lax.axis_index("ctx")

    def frame(device):
        return perm_ref[device * local_slots + part * (local_slots // 2)] // frame_rows

    frames = [frame(me ^ m) for m in range(2 * masked)]
    for h in range(heads):
        cols = pl.ds(h * HD, HD)
        wide_cols = pl.ds(2 * h * HD, 2 * HD)
        for r in sides:
            window = pl.ds(r * rows, rows)
            target = window if len(sides) == 2 else slice(None)
            q = q_ref[window, cols]
            if carried:
                acc = state_ref[window, wide_cols]
            else:
                acc = jnp.zeros((rows, 2 * HD), jnp.float32)
            for i in range(free + masked):
                keys = kv[i][:, cols]
                values = kv[i][:, pl.ds(width + h * HD, HD)]
                scores = lax.dot_general(
                    q, keys, (((1,), (1,)), ((), ())), preferred_element_type=jnp.float32
                )
                if i >= free:
                    half = scores.shape[1] // 2
                    at = 2 * (i - free)
                    bias = [
                        jnp.where(frames[at + s] <= frames[r], jnp.float32(0), jnp.float32(MASKED))
                        for s in range(2)
                    ]
                    scores = jnp.concatenate(
                        [scores[:, :half] + bias[0], scores[:, half:] + bias[1]], axis=1
                    )
                weights = jnp.exp2(scores).astype(jnp.bfloat16)
                wide = jnp.concatenate([values, jnp.ones_like(values)], axis=1)
                acc += jnp.dot(weights, wide, preferred_element_type=jnp.float32)
            if final:
                out_ref[target, cols] = (acc[:, :HD] / acc[:, HD:]).astype(jnp.bfloat16)
            else:
                out_ref[target, wide_cols] = acc


def attend(block_perm, q, state, free, masked, part, local_slots, sides, final):
    rows2, width = q.shape
    heads = width // HD
    keys = sum(p.shape[0] for p in free + masked)
    carried = 0 if state is None else 1
    out_rows = rows2 * len(sides) // 2
    if final:
        out = jax.ShapeDtypeStruct((out_rows, width), jnp.bfloat16)
    else:
        out = jax.ShapeDtypeStruct((out_rows, 2 * width), jnp.float32)
    return vmem_call(
        functools.partial(
            attend_kernel, carried, sides, final, len(free), len(masked), heads, part, local_slots
        ),
        [q] + ([state] if carried else []) + free + masked,
        [out],
        smem=[block_perm],
        flops=8 * out_rows * keys * width,
    )


def output_kernel(shifts, mine_ref, theirs_ref, w_ref, *outs):
    levels = len(shifts)
    rows = theirs_ref.shape[0]
    width = mine_ref.shape[1]
    level = lax.axis_index("head")
    core = lax.axis_index("ctx") % CORES
    mine_at = pl.ds(pl.multiple_of(core * width, width), width)
    theirs_at = pl.ds(pl.multiple_of((1 - core) * width, width), width)
    mine = mine_ref[pl.ds(0, rows), :]
    theirs = theirs_ref[...]
    span = w_ref.shape[1] // levels
    for i, k in enumerate(shifts):
        block = level ^ k
        cols = pl.ds(pl.multiple_of(block * span, span), span)
        part = jnp.dot(mine, w_ref[mine_at, cols], preferred_element_type=jnp.float32)
        part += jnp.dot(theirs, w_ref[theirs_at, cols], preferred_element_type=jnp.float32)
        outs[i][...] = part.astype(outs[i].dtype)


def output_parts(shifts, mine, theirs, w_out):
    rows = theirs.shape[0]
    cols = w_out.shape[1] // len(shifts)
    return vmem_call(
        functools.partial(output_kernel, shifts),
        [mine, theirs, w_out],
        [
            jax.ShapeDtypeStruct((rows, cols), jnp.float32 if k == 0 else jnp.bfloat16)
            for k in shifts
        ],
        flops=2 * rows * w_out.shape[0] * w_out.shape[1],
    )


def finish_kernel(count, *refs):
    out_ref = refs[-1]
    rows = refs[0].shape[0]
    for part in range(2):
        group = refs[part * count : (part + 1) * count]
        total = group[0][...]
        for ref in group[1:]:
            total += ref[...].astype(jnp.float32)
        out_ref[pl.ds(part * rows, rows), :] = total.astype(out_ref.dtype)


def finish(first, second):
    rows, cols = first[0].shape
    return vmem_call(
        functools.partial(finish_kernel, len(first)),
        [*first, *second],
        [jax.ShapeDtypeStruct((2 * rows, cols), jnp.bfloat16)],
        flops=rows * cols,
    )


def per_device(ctx, levels, tokens, w_qkv, w_out, block_perm):
    rows = tokens.shape[0]
    half = rows // 2
    local_slots = rows // WW
    run_slots = local_slots // 2
    me = lax.axis_index("ctx")
    chips = ctx // CORES
    frame_rows = block_perm.shape[0] // F
    slot_frame = block_perm // frame_rows
    slot_row = block_perm % frame_rows

    shifts = list(range(levels - 1, 0, -1))

    def over_levels(x, k):
        return lax.ppermute(x, "head", [(i, i ^ k) for i in range(levels)])

    def over_ctx(x, mask):
        return lax.ppermute(x, "ctx", [(i, i ^ mask) for i in range(ctx)])

    def slots_of(values, device, part):
        first = device * local_slots + part * run_slots
        return lax.dynamic_slice_in_dim(values, first, run_slots)

    def tables(part):
        frame = jnp.concatenate([slots_of(slot_frame, me, part), slots_of(slot_frame, me ^ 1, part)])
        row = jnp.concatenate([slots_of(slot_row, me, part), slots_of(slot_row, me ^ 1, part)])
        return rope_tables(frame, row)

    turns = [tables(part) for part in range(2)]
    gathered = []
    held = None
    for part in range(2):
        if held is not None:
            tokens, gathered[0][1:] = lax.optimization_barrier((tokens, held))
        own = tokens[part * half : (part + 1) * half]
        pieces = [own]
        for k in shifts:
            pieces.append(over_levels(own, k))
        held = pieces[1:]
        gathered.append(pieces)
    w_mine = fetch(w_qkv)
    last, turns, w_mine = lax.optimization_barrier((gathered[0][-1], turns, w_mine))
    gathered[0][-1] = last

    projected = []
    for part in range(2):
        mine = gathered[part]
        if part == 1:
            mine[1:], q = lax.optimization_barrier((mine[1:], q))
            projected[0] = (q, pieces)
        theirs = []
        for piece in mine:
            theirs.append(over_ctx(piece, 1))
        inputs = ([0] + shifts, mine, theirs, w_mine, *turns[part])
        kv = project("kv", *inputs)
        pieces = [kv]
        for m in range(1, chips):
            pieces.append(over_ctx(kv, 2 * m))
        q = project("q", *inputs)
        projected.append((q, pieces))
    sums = []
    for part in range(2):
        q, pieces = projected[part]
        state = None
        if part == 1:
            state = attend(block_perm, q, None, projected[0][1], [], part, local_slots, (0, 1), False)
            pieces[1:], state = lax.optimization_barrier((pieces[1:], state))
        both = []
        for side in (1, 0):
            both.append(attend(block_perm, q, state, [], pieces, part, local_slots, (side,), True))
            if side == 1:
                theirs = over_ctx(both[0], 1)
        heads_out = both[1]
        parts = output_parts(shifts + [0], heads_out, theirs, w_out)
        arrived = []
        for k, p in zip(shifts, parts):
            arrived.append(over_levels(p, k))
        sums.append([parts[-1]] + arrived)
    return finish(*sums)


def solution(mesh):
    in_specs = (P("ctx", "head"), P(None, None, "head"), P("head", None), P())
    out_specs = P("ctx", "head")

    def body(*args):
        return per_device(mesh.shape["ctx"], mesh.shape["head"], *args)

    return jax.shard_map(
        body, mesh=mesh, in_specs=in_specs, out_specs=out_specs, check_vma=False
    )
```

```python
import functools
import math

import jax
import jax.numpy as jnp
from jax import lax
from jax.experimental import pallas as pl
from jax.experimental.pallas import tpu as pltpu
from jax.sharding import PartitionSpec as P


HD = 128
WW = 64
F = 8
ROPE_BASE = 10000.0
EPSILON = 1e-06
CORES = 2
MASKED = -1e30
GRANT = 12 << 20


def part_sizes():
    return (HD // 16, 7 * HD // 32, 7 * HD // 32)


def rope_tables(slot_frame, slot_row):
    slots = slot_frame.shape[0]
    lane = lax.broadcasted_iota(jnp.int32, (slots, WW, HD), 2)
    column = lax.broadcasted_iota(jnp.int32, (slots, WW, HD), 1).astype(jnp.float32)
    frame = jnp.broadcast_to(slot_frame.astype(jnp.float32)[:, None, None], lane.shape)
    row = jnp.broadcast_to(slot_row.astype(jnp.float32)[:, None, None], lane.shape)
    p0, p1, p2 = part_sizes()
    first, second = 2 * p0, 2 * p0 + 2 * p1
    position = jnp.where(lane < first, frame, jnp.where(lane < second, row, column))
    freq, sign = [], []
    for pairs in (p0, p1, p2):
        steps = ROPE_BASE ** (-jnp.arange(pairs, dtype=jnp.float32) / pairs)
        freq += [steps, steps]
        sign += [-jnp.ones((pairs,), jnp.float32), jnp.ones((pairs,), jnp.float32)]
    angle = position * jnp.concatenate(freq)
    cosine = jnp.cos(angle).reshape(slots * WW, HD)
    sine = (jnp.sin(angle) * jnp.concatenate(sign)).reshape(slots * WW, HD)
    return cosine, sine


def norm_rotate(v, cosine, sine, scale):
    p0, p1, _ = part_sizes()
    mean = jnp.mean(v * v, axis=-1, keepdims=True)
    v = v * (lax.rsqrt(mean + EPSILON) * scale)
    lane = lax.broadcasted_iota(jnp.int32, v.shape, 1)
    low = (
        (lane < p0)
        | ((lane >= 2 * p0) & (lane < 2 * p0 + p1))
        | ((lane >= 2 * p0 + 2 * p1) & (lane < 2 * p0 + 3 * p1))
    )
    near = jnp.where(low, pltpu.roll(v, HD - p0, 1), pltpu.roll(v, p0, 1))
    far = jnp.where(low, pltpu.roll(v, HD - p1, 1), pltpu.roll(v, p1, 1))
    other = jnp.where(lane < 2 * p0, near, far)
    return v * cosine + other * sine


def vmem_call(body, inputs, outputs, smem=(), after=(), scratch=(), flops=0, grant=GRANT):
    vmem = pl.BlockSpec(memory_space=pltpu.VMEM)
    n_smem, n_after = len(smem), len(after)

    def kernel(*refs):
        body(*refs[:n_smem], *refs[n_smem + n_after :])

    single = len(outputs) == 1
    return pl.pallas_call(
        kernel,
        in_specs=[pl.BlockSpec(memory_space=pltpu.SMEM)] * n_smem
        + [pl.BlockSpec(memory_space=pl.ANY)] * n_after
        + [vmem] * len(inputs),
        out_specs=vmem if single else [vmem] * len(outputs),
        out_shape=outputs[0] if single else list(outputs),
        scratch_shapes=list(scratch),
        compiler_params=pltpu.CompilerParams(vmem_limit_bytes=grant),
        cost_estimate=pl.CostEstimate(flops=flops, bytes_accessed=0, transcendentals=0),
    )(*smem, *after, *inputs)


def fetch_kernel(w_ref, out_ref, sems):
    width = out_ref.shape[2]
    core = lax.axis_index("ctx") % CORES
    cols = pl.ds(pl.multiple_of(core * width, width), width)
    copies = [
        pltpu.make_async_copy(w_ref.at[at, :, cols], out_ref.at[at], sems.at[at])
        for at in range(out_ref.shape[0])
    ]
    for copy in copies:
        copy.start()
    for copy in copies:
        copy.wait()


def fetch(w_qkv):
    three, feats, cols = w_qkv.shape
    return pl.pallas_call(
        fetch_kernel,
        in_specs=[pl.BlockSpec(memory_space=pltpu.MemorySpace.HBM)],
        out_specs=pl.BlockSpec(memory_space=pltpu.VMEM),
        out_shape=jax.ShapeDtypeStruct((three, feats, cols // CORES), jnp.bfloat16),
        scratch_shapes=[pltpu.SemaphoreType.DMA((three,))],
        compiler_params=pltpu.CompilerParams(vmem_limit_bytes=46 << 20),
        name="fetch",
    )(w_qkv)


def project_kernel(pieces, heads, shifts, kind, cos_ref, sin_ref, *refs):
    mine = refs[:pieces]
    theirs = refs[pieces : 2 * pieces]
    w_ref, out_ref = refs[2 * pieces :]
    _, feats = mine[0].shape
    width = heads * HD
    level = lax.axis_index("head")

    def product(j):
        total = None
        for i, k in enumerate(shifts):
            block = level ^ k
            at = pl.ds(pl.multiple_of(block * feats, feats), feats)
            x = jnp.concatenate([mine[i][...], theirs[i][...]], axis=0)
            dot = jnp.dot(x, w_ref[j, at, :], preferred_element_type=jnp.float32)
            total = dot if total is None else total + dot
        return total

    scale = HD ** (-0.5) * math.log2(math.e) if kind == "q" else 1.0
    raw = product(0 if kind == "q" else 1)
    if kind == "kv":
        out_ref[:, pl.ds(width, width)] = product(2).astype(jnp.bfloat16)
    cosine, sine = cos_ref[...], sin_ref[...]
    for h in range(heads):
        v = norm_rotate(raw[:, h * HD : (h + 1) * HD], cosine, sine, scale)
        out_ref[:, pl.ds(h * HD, HD)] = v.astype(jnp.bfloat16)


def project(kind, shifts, mine, theirs, w_qkv, cosine, sine):
    pieces = len(mine)
    rows, feats = mine[0].shape
    width = w_qkv.shape[2]
    count = 1 if kind == "q" else 2
    return vmem_call(
        functools.partial(project_kernel, pieces, width // HD, shifts, kind),
        [cosine, sine, *mine, *theirs, w_qkv],
        [jax.ShapeDtypeStruct((2 * rows, count * width), jnp.bfloat16)],
        flops=2 * 2 * rows * feats * pieces * count * width,
    )


def attend_kernel(
    carried, sides, final, free, masked, heads, part, local_slots, perm_ref, q_ref, *refs
):
    state_ref = refs[0] if carried else None
    kv = refs[carried : carried + free + masked]
    out_ref = refs[-1]
    rows = q_ref.shape[0] // 2
    width = heads * HD
    frame_rows = perm_ref.shape[0] // F
    me = lax.axis_index("ctx")

    def frame(device):
        return perm_ref[device * local_slots + part * (local_slots // 2)] // frame_rows

    frames = [frame(me ^ m) for m in range(2 * masked)]

    def weights_of(h, r):
        q = q_ref[pl.ds(r * rows, rows), pl.ds(h * HD, HD)]
        found = []
        for i in range(free + masked):
            scores = lax.dot_general(
                q,
                kv[i][:, pl.ds(h * HD, HD)],
                (((1,), (1,)), ((), ())),
                preferred_element_type=jnp.float32,
            )
            if i >= free:
                half = scores.shape[1] // 2
                at = 2 * (i - free)
                bias = [
                    jnp.where(frames[at + s] <= frames[r], jnp.float32(0), jnp.float32(MASKED))
                    for s in range(2)
                ]
                scores = jnp.concatenate(
                    [scores[:, :half] + bias[0], scores[:, half:] + bias[1]], axis=1
                )
            found.append(jnp.exp2(scores).astype(jnp.bfloat16))
        return found

    def finish_head(h, r, weights):
        wide_cols = pl.ds(2 * h * HD, 2 * HD)
        window = pl.ds(r * rows, rows)
        target = window if len(sides) == 2 else slice(None)
        acc = None
        for i in range(free + masked):
            values = kv[i][:, pl.ds(width + h * HD, HD)]
            wide = jnp.concatenate([values, jnp.ones_like(values)], axis=1)
            dot = jnp.dot(weights[i], wide, preferred_element_type=jnp.float32)
            acc = dot if acc is None else acc + dot
        if carried:
            acc = acc + state_ref[window, wide_cols]
        if final:
            out_ref[target, pl.ds(h * HD, HD)] = (acc[:, :HD] / acc[:, HD:]).astype(jnp.bfloat16)
        else:
            out_ref[target, wide_cols] = acc

    pending = None
    for h in range(heads):
        for r in sides:
            weights = weights_of(h, r)
            if pending is not None:
                finish_head(*pending)
            pending = (h, r, weights)
    finish_head(*pending)


def attend(block_perm, q, state, free, masked, part, local_slots, sides, final):
    rows2, width = q.shape
    heads = width // HD
    keys = sum(p.shape[0] for p in free + masked)
    carried = 0 if state is None else 1
    out_rows = rows2 * len(sides) // 2
    if final:
        out = jax.ShapeDtypeStruct((out_rows, width), jnp.bfloat16)
    else:
        out = jax.ShapeDtypeStruct((out_rows, 2 * width), jnp.float32)
    return vmem_call(
        functools.partial(
            attend_kernel, carried, sides, final, len(free), len(masked), heads, part, local_slots
        ),
        [q] + ([state] if carried else []) + free + masked,
        [out],
        smem=[block_perm],
        flops=8 * out_rows * keys * width,
    )


def output_kernel(shifts, mine_ref, theirs_ref, w_ref, *outs):
    levels = len(shifts)
    rows = theirs_ref.shape[0]
    width = mine_ref.shape[1]
    level = lax.axis_index("head")
    core = lax.axis_index("ctx") % CORES
    mine_at = pl.ds(pl.multiple_of(core * width, width), width)
    theirs_at = pl.ds(pl.multiple_of((1 - core) * width, width), width)
    mine = mine_ref[pl.ds(0, rows), :]
    theirs = theirs_ref[...]
    span = w_ref.shape[1] // levels
    for i, k in enumerate(shifts):
        block = level ^ k
        cols = pl.ds(pl.multiple_of(block * span, span), span)
        part = jnp.dot(mine, w_ref[mine_at, cols], preferred_element_type=jnp.float32)
        part += jnp.dot(theirs, w_ref[theirs_at, cols], preferred_element_type=jnp.float32)
        outs[i][...] = part.astype(outs[i].dtype)


def output_parts(shifts, mine, theirs, w_out):
    rows = theirs.shape[0]
    cols = w_out.shape[1] // len(shifts)
    return vmem_call(
        functools.partial(output_kernel, shifts),
        [mine, theirs, w_out],
        [
            jax.ShapeDtypeStruct((rows, cols), jnp.float32 if k == 0 else jnp.bfloat16)
            for k in shifts
        ],
        flops=2 * rows * w_out.shape[0] * w_out.shape[1],
    )


def finish_kernel(count, *refs):
    out_ref = refs[-1]
    rows = refs[0].shape[0]
    for part in range(2):
        group = refs[part * count : (part + 1) * count]
        total = group[0][...]
        for ref in group[1:]:
            total += ref[...].astype(jnp.float32)
        out_ref[pl.ds(part * rows, rows), :] = total.astype(out_ref.dtype)


def finish(first, second):
    rows, cols = first[0].shape
    return vmem_call(
        functools.partial(finish_kernel, len(first)),
        [*first, *second],
        [jax.ShapeDtypeStruct((2 * rows, cols), jnp.bfloat16)],
        flops=rows * cols,
    )


def per_device(ctx, levels, tokens, w_qkv, w_out, block_perm):
    rows = tokens.shape[0]
    half = rows // 2
    local_slots = rows // WW
    run_slots = local_slots // 2
    me = lax.axis_index("ctx")
    chips = ctx // CORES
    frame_rows = block_perm.shape[0] // F
    slot_frame = block_perm // frame_rows
    slot_row = block_perm % frame_rows

    shifts = list(range(levels - 1, 0, -1))

    def over_levels(x, k):
        return lax.ppermute(x, "head", [(i, i ^ k) for i in range(levels)])

    def over_ctx(x, mask):
        return lax.ppermute(x, "ctx", [(i, i ^ mask) for i in range(ctx)])

    def slots_of(values, device, part):
        first = device * local_slots + part * run_slots
        return lax.dynamic_slice_in_dim(values, first, run_slots)

    def tables(part):
        frame = jnp.concatenate([slots_of(slot_frame, me, part), slots_of(slot_frame, me ^ 1, part)])
        row = jnp.concatenate([slots_of(slot_row, me, part), slots_of(slot_row, me ^ 1, part)])
        return rope_tables(frame, row)

    turns = [tables(part) for part in range(2)]
    gathered = []
    held = None
    for part in range(2):
        if held is not None:
            tokens, gathered[0][1:] = lax.optimization_barrier((tokens, held))
        own = tokens[part * half : (part + 1) * half]
        pieces = [own]
        for k in shifts:
            pieces.append(over_levels(own, k))
        held = pieces[1:]
        gathered.append(pieces)
    w_mine = fetch(w_qkv)
    last, turns, w_mine = lax.optimization_barrier((gathered[0][-1], turns, w_mine))
    gathered[0][-1] = last

    projected = []
    for part in range(2):
        mine = gathered[part]
        if part == 1:
            mine[1:], q = lax.optimization_barrier((mine[1:], q))
            projected[0] = (q, pieces)
        theirs = []
        for piece in mine:
            theirs.append(over_ctx(piece, 1))
        inputs = ([0] + shifts, mine, theirs, w_mine, *turns[part])
        kv = project("kv", *inputs)
        pieces = [kv]
        for m in range(1, chips):
            pieces.append(over_ctx(kv, 2 * m))
        q = project("q", *inputs)
        projected.append((q, pieces))
    sums = []
    for part in range(2):
        q, pieces = projected[part]
        state = None
        if part == 1:
            state = attend(block_perm, q, None, projected[0][1], [], part, local_slots, (0, 1), False)
            pieces[1:], state = lax.optimization_barrier((pieces[1:], state))
        both = []
        for side in (1, 0):
            both.append(attend(block_perm, q, state, [], pieces, part, local_slots, (side,), True))
            if side == 1:
                theirs = over_ctx(both[0], 1)
        heads_out = both[1]
        parts = output_parts(shifts + [0], heads_out, theirs, w_out)
        arrived = []
        for k, p in zip(shifts, parts):
            arrived.append(over_levels(p, k))
        sums.append([parts[-1]] + arrived)
    return finish(*sums)


def solution(mesh):
    in_specs = (P("ctx", "head"), P(None, None, "head"), P("head", None), P())
    out_specs = P("ctx", "head")

    def body(*args):
        return per_device(mesh.shape["ctx"], mesh.shape["head"], *args)

    return jax.shard_map(
        body, mesh=mesh, in_specs=in_specs, out_specs=out_specs, check_vma=False
    )
```

```python
import functools
import math

import jax
import jax.numpy as jnp
from jax import lax
from jax.experimental import pallas as pl
from jax.experimental.pallas import tpu as pltpu
from jax.sharding import PartitionSpec as P


HD = 128
WW = 64
F = 8
ROPE_BASE = 10000.0
EPSILON = 1e-06
CORES = 2
MASKED = -1e30
GRANT = 12 << 20


def part_sizes():
    return (HD // 16, 7 * HD // 32, 7 * HD // 32)


def rope_tables(slot_frame, slot_row):
    slots = slot_frame.shape[0]
    lane = lax.broadcasted_iota(jnp.int32, (slots, WW, HD), 2)
    column = lax.broadcasted_iota(jnp.int32, (slots, WW, HD), 1).astype(jnp.float32)
    frame = jnp.broadcast_to(slot_frame.astype(jnp.float32)[:, None, None], lane.shape)
    row = jnp.broadcast_to(slot_row.astype(jnp.float32)[:, None, None], lane.shape)
    p0, p1, p2 = part_sizes()
    first, second = 2 * p0, 2 * p0 + 2 * p1
    position = jnp.where(lane < first, frame, jnp.where(lane < second, row, column))
    freq, sign = [], []
    for pairs in (p0, p1, p2):
        steps = ROPE_BASE ** (-jnp.arange(pairs, dtype=jnp.float32) / pairs)
        freq += [steps, steps]
        sign += [-jnp.ones((pairs,), jnp.float32), jnp.ones((pairs,), jnp.float32)]
    angle = position * jnp.concatenate(freq)
    cosine = jnp.cos(angle).reshape(slots * WW, HD)
    sine = (jnp.sin(angle) * jnp.concatenate(sign)).reshape(slots * WW, HD)
    return cosine, sine


def norm_rotate(v, cosine, sine, scale):
    p0, p1, _ = part_sizes()
    mean = jnp.mean(v * v, axis=-1, keepdims=True)
    v = v * (lax.rsqrt(mean + EPSILON) * scale)
    lane = lax.broadcasted_iota(jnp.int32, v.shape, 1)
    low = (
        (lane < p0)
        | ((lane >= 2 * p0) & (lane < 2 * p0 + p1))
        | ((lane >= 2 * p0 + 2 * p1) & (lane < 2 * p0 + 3 * p1))
    )
    near = jnp.where(low, pltpu.roll(v, HD - p0, 1), pltpu.roll(v, p0, 1))
    far = jnp.where(low, pltpu.roll(v, HD - p1, 1), pltpu.roll(v, p1, 1))
    other = jnp.where(lane < 2 * p0, near, far)
    return v * cosine + other * sine


def vmem_call(body, inputs, outputs, smem=(), after=(), scratch=(), flops=0, grant=GRANT):
    vmem = pl.BlockSpec(memory_space=pltpu.VMEM)
    n_smem, n_after = len(smem), len(after)

    def kernel(*refs):
        body(*refs[:n_smem], *refs[n_smem + n_after :])

    single = len(outputs) == 1
    return pl.pallas_call(
        kernel,
        in_specs=[pl.BlockSpec(memory_space=pltpu.SMEM)] * n_smem
        + [pl.BlockSpec(memory_space=pl.ANY)] * n_after
        + [vmem] * len(inputs),
        out_specs=vmem if single else [vmem] * len(outputs),
        out_shape=outputs[0] if single else list(outputs),
        scratch_shapes=list(scratch),
        compiler_params=pltpu.CompilerParams(vmem_limit_bytes=grant),
        cost_estimate=pl.CostEstimate(flops=flops, bytes_accessed=0, transcendentals=0),
    )(*smem, *after, *inputs)


def fetch_kernel(w_ref, out_ref, sems):
    width = out_ref.shape[2]
    core = lax.axis_index("ctx") % CORES
    cols = pl.ds(pl.multiple_of(core * width, width), width)
    copies = [
        pltpu.make_async_copy(w_ref.at[at, :, cols], out_ref.at[at], sems.at[at])
        for at in range(out_ref.shape[0])
    ]
    for copy in copies:
        copy.start()
    for copy in copies:
        copy.wait()


def fetch(w_qkv):
    three, feats, cols = w_qkv.shape
    return pl.pallas_call(
        fetch_kernel,
        in_specs=[pl.BlockSpec(memory_space=pltpu.MemorySpace.HBM)],
        out_specs=pl.BlockSpec(memory_space=pltpu.VMEM),
        out_shape=jax.ShapeDtypeStruct((three, feats, cols // CORES), jnp.bfloat16),
        scratch_shapes=[pltpu.SemaphoreType.DMA((three,))],
        compiler_params=pltpu.CompilerParams(vmem_limit_bytes=46 << 20),
        name="fetch",
    )(w_qkv)


def project_kernel(pieces, heads, shifts, kind, cos_ref, sin_ref, *refs):
    mine = refs[:pieces]
    theirs = refs[pieces : 2 * pieces]
    w_ref, out_ref = refs[2 * pieces :]
    _, feats = mine[0].shape
    width = heads * HD
    level = lax.axis_index("head")

    def product(j):
        total = None
        for i, k in enumerate(shifts):
            block = level ^ k
            at = pl.ds(pl.multiple_of(block * feats, feats), feats)
            x = jnp.concatenate([mine[i][...], theirs[i][...]], axis=0)
            dot = jnp.dot(x, w_ref[j, at, :], preferred_element_type=jnp.float32)
            total = dot if total is None else total + dot
        return total

    scale = HD ** (-0.5) * math.log2(math.e) if kind == "q" else 1.0
    raw = product(0 if kind == "q" else 1)
    if kind == "kv":
        out_ref[:, pl.ds(width, width)] = product(2).astype(jnp.bfloat16)
    cosine, sine = cos_ref[...], sin_ref[...]
    for h in range(heads):
        v = norm_rotate(raw[:, h * HD : (h + 1) * HD], cosine, sine, scale)
        out_ref[:, pl.ds(h * HD, HD)] = v.astype(jnp.bfloat16)


def project(kind, shifts, mine, theirs, w_qkv, cosine, sine):
    pieces = len(mine)
    rows, feats = mine[0].shape
    width = w_qkv.shape[2]
    count = 1 if kind == "q" else 2
    return vmem_call(
        functools.partial(project_kernel, pieces, width // HD, shifts, kind),
        [cosine, sine, *mine, *theirs, w_qkv],
        [jax.ShapeDtypeStruct((2 * rows, count * width), jnp.bfloat16)],
        flops=2 * 2 * rows * feats * pieces * count * width,
    )


def attend_kernel(
    carried, sides, final, free, masked, start, heads, part, local_slots, perm_ref, q_ref, *refs
):
    state_ref = refs[0] if carried else None
    kv = refs[carried : carried + free + masked]
    out_ref = refs[-1]
    rows = q_ref.shape[0] // 2
    width = heads * HD
    frame_rows = perm_ref.shape[0] // F
    me = lax.axis_index("ctx")

    def frame(device):
        return perm_ref[device * local_slots + part * (local_slots // 2)] // frame_rows

    asking = [frame(me ^ m) for m in range(2)]
    frames = [frame(me ^ (2 * start + m)) for m in range(2 * masked)]

    def weights_of(h, r):
        q = q_ref[pl.ds(r * rows, rows), pl.ds(h * HD, HD)]
        found = []
        for i in range(free + masked):
            scores = lax.dot_general(
                q,
                kv[i][:, pl.ds(h * HD, HD)],
                (((1,), (1,)), ((), ())),
                preferred_element_type=jnp.float32,
            )
            if i >= free:
                half = scores.shape[1] // 2
                at = 2 * (i - free)
                bias = [
                    jnp.where(frames[at + s] <= asking[r], jnp.float32(0), jnp.float32(MASKED))
                    for s in range(2)
                ]
                scores = jnp.concatenate(
                    [scores[:, :half] + bias[0], scores[:, half:] + bias[1]], axis=1
                )
            found.append(jnp.exp2(scores).astype(jnp.bfloat16))
        return found

    def finish_head(h, r, weights):
        wide_cols = pl.ds(2 * h * HD, 2 * HD)
        window = pl.ds(r * rows, rows)
        target = window if len(sides) == 2 else slice(None)
        acc = None
        for i in range(free + masked):
            values = kv[i][:, pl.ds(width + h * HD, HD)]
            wide = jnp.concatenate([values, jnp.ones_like(values)], axis=1)
            dot = jnp.dot(weights[i], wide, preferred_element_type=jnp.float32)
            acc = dot if acc is None else acc + dot
        if carried:
            acc = acc + state_ref[window, wide_cols]
        if final:
            out_ref[target, pl.ds(h * HD, HD)] = (acc[:, :HD] / acc[:, HD:]).astype(jnp.bfloat16)
        else:
            out_ref[target, wide_cols] = acc

    pending = None
    for h in range(heads):
        for r in sides:
            weights = weights_of(h, r)
            if pending is not None:
                finish_head(*pending)
            pending = (h, r, weights)
    finish_head(*pending)


def attend(block_perm, q, state, free, masked, start, part, local_slots, sides, final):
    rows2, width = q.shape
    heads = width // HD
    keys = sum(p.shape[0] for p in free + masked)
    carried = 0 if state is None else 1
    out_rows = rows2 * len(sides) // 2
    if final:
        out = jax.ShapeDtypeStruct((out_rows, width), jnp.bfloat16)
    else:
        out = jax.ShapeDtypeStruct((out_rows, 2 * width), jnp.float32)
    return vmem_call(
        functools.partial(
            attend_kernel, carried, sides, final, len(free), len(masked), start, heads, part, local_slots
        ),
        [q] + ([state] if carried else []) + free + masked,
        [out],
        smem=[block_perm],
        flops=8 * out_rows * keys * width,
    )


def output_kernel(shifts, mine_ref, theirs_ref, w_ref, *outs):
    levels = len(shifts)
    rows = theirs_ref.shape[0]
    width = mine_ref.shape[1]
    level = lax.axis_index("head")
    core = lax.axis_index("ctx") % CORES
    mine_at = pl.ds(pl.multiple_of(core * width, width), width)
    theirs_at = pl.ds(pl.multiple_of((1 - core) * width, width), width)
    mine = mine_ref[pl.ds(0, rows), :]
    theirs = theirs_ref[...]
    span = w_ref.shape[1] // levels
    for i, k in enumerate(shifts):
        block = level ^ k
        cols = pl.ds(pl.multiple_of(block * span, span), span)
        part = jnp.dot(mine, w_ref[mine_at, cols], preferred_element_type=jnp.float32)
        part += jnp.dot(theirs, w_ref[theirs_at, cols], preferred_element_type=jnp.float32)
        outs[i][...] = part.astype(outs[i].dtype)


def output_parts(shifts, mine, theirs, w_out):
    rows = theirs.shape[0]
    cols = w_out.shape[1] // len(shifts)
    return vmem_call(
        functools.partial(output_kernel, shifts),
        [mine, theirs, w_out],
        [
            jax.ShapeDtypeStruct((rows, cols), jnp.float32 if k == 0 else jnp.bfloat16)
            for k in shifts
        ],
        flops=2 * rows * w_out.shape[0] * w_out.shape[1],
    )


def finish_kernel(count, *refs):
    out_ref = refs[-1]
    rows = refs[0].shape[0]
    for part in range(2):
        group = refs[part * count : (part + 1) * count]
        total = group[0][...]
        for ref in group[1:]:
            total += ref[...].astype(jnp.float32)
        out_ref[pl.ds(part * rows, rows), :] = total.astype(out_ref.dtype)


def finish(first, second):
    rows, cols = first[0].shape
    return vmem_call(
        functools.partial(finish_kernel, len(first)),
        [*first, *second],
        [jax.ShapeDtypeStruct((2 * rows, cols), jnp.bfloat16)],
        flops=rows * cols,
    )


def per_device(ctx, levels, tokens, w_qkv, w_out, block_perm):
    rows = tokens.shape[0]
    half = rows // 2
    local_slots = rows // WW
    run_slots = local_slots // 2
    me = lax.axis_index("ctx")
    chips = ctx // CORES
    frame_rows = block_perm.shape[0] // F
    slot_frame = block_perm // frame_rows
    slot_row = block_perm % frame_rows

    shifts = list(range(levels - 1, 0, -1))

    def over_levels(x, k):
        return lax.ppermute(x, "head", [(i, i ^ k) for i in range(levels)])

    def over_ctx(x, mask):
        return lax.ppermute(x, "ctx", [(i, i ^ mask) for i in range(ctx)])

    def slots_of(values, device, part):
        first = device * local_slots + part * run_slots
        return lax.dynamic_slice_in_dim(values, first, run_slots)

    def tables(part):
        frame = jnp.concatenate([slots_of(slot_frame, me, part), slots_of(slot_frame, me ^ 1, part)])
        row = jnp.concatenate([slots_of(slot_row, me, part), slots_of(slot_row, me ^ 1, part)])
        return rope_tables(frame, row)

    turns = [tables(part) for part in range(2)]
    gathered = []
    held = None
    for part in range(2):
        if held is not None:
            tokens, gathered[0][1:] = lax.optimization_barrier((tokens, held))
        own = tokens[part * half : (part + 1) * half]
        pieces = [own]
        for k in shifts:
            pieces.append(over_levels(own, k))
        held = pieces[1:]
        gathered.append(pieces)
    w_mine = fetch(w_qkv)
    last, turns, w_mine = lax.optimization_barrier((gathered[0][-1], turns, w_mine))
    gathered[0][-1] = last

    projected = []
    for part in range(2):
        mine = gathered[part]
        if part == 1:
            mine[1:], q = lax.optimization_barrier((mine[1:], q))
            projected[0] = (q, pieces)
        theirs = []
        for piece in mine:
            theirs.append(over_ctx(piece, 1))
        inputs = ([0] + shifts, mine, theirs, w_mine, *turns[part])
        kv = project("kv", *inputs)
        pieces = [kv]
        for m in range(1, chips):
            pieces.append(over_ctx(kv, 2 * m))
        q = project("q", *inputs)
        projected.append((q, pieces))
    sums = []
    for part in range(2):
        q, pieces = projected[part]
        state = None
        if part == 1:
            state = attend(block_perm, q, None, projected[0][1], pieces[:1], 0, part, local_slots, (0, 1), False)
            pieces[1:], state = lax.optimization_barrier((pieces[1:], state))
        both = []
        for side in (1, 0):
            both.append(
                attend(block_perm, q, state, [], pieces[part:], part, part, local_slots, (side,), True)
            )
            if side == 1:
                theirs = over_ctx(both[0], 1)
        heads_out = both[1]
        parts = output_parts(shifts + [0], heads_out, theirs, w_out)
        arrived = []
        for k, p in zip(shifts, parts):
            arrived.append(over_levels(p, k))
        sums.append([parts[-1]] + arrived)
    return finish(*sums)


def solution(mesh):
    in_specs = (P("ctx", "head"), P(None, None, "head"), P("head", None), P())
    out_specs = P("ctx", "head")

    def body(*args):
        return per_device(mesh.shape["ctx"], mesh.shape["head"], *args)

    return jax.shard_map(
        body, mesh=mesh, in_specs=in_specs, out_specs=out_specs, check_vma=False
    )
```
